32 devices in a mesh: cuts: 2 (over y), blk: 4 (over z), sol: 4 (over x, core).
Axes of the slice: x: 2, y: 2, z: 4, core: 2. Of those that a mesh axis runs over, the one named last changes fastest.
Arguments:
- solutions: bfloat16 [20, 2, 3, 256, 4096], P('cuts', None, None, None, ('blk', 'sol')), parts along dimension 0, may hold values from -6 to 6
- eigvecs: bfloat16 [20, 2, 3, 128, 4096], P('cuts', None, None, None, ('blk', 'sol')), parts along dimension 0, may hold values from -430 to 430
Outputs:
- projected: float32 [128, 20, 2, 256], P(('blk', 'sol'), 'cuts'), parts along dimension 1
The draws below stay inside these ranges and needn't reach their ends.
There are 2 independent parts, one for each index of `cuts`. The reference program is written for one: setup_inputs(seed, part) draws one part's arguments, and reference() takes and returns one part's arrays. A program takes and returns all parts, laid end to end along the dimension named above; each array names one. Nothing has to cross between parts.
All inputs are finite; a program needn't handle non-finite values.
Results may differ from the reference program's by a relative error of at most 0.0003.
Values sent between devices are 32-bit elements; how exact they have to be, the bound alone decides.
No kernel may reach another device: no remote copies, remote signals or barrier semaphores. Data moves between devices by JAX's collectives and lax.ppermute only.
A program may use at most 64 MiB of HBM per device.

```python
import math
import jax
import jax.numpy as jnp
from jax import lax

TS = 10
K = 128
COLORS = 3
NCOL = 256
SITES = 4096


def draw_eigvecs(key, part):
    key_base = jax.random.fold_in(key, 11)
    key_gain = jax.random.fold_in(key, 12)
    key_phase = jax.random.fold_in(key, 13)
    shape = (TS, 2, COLORS, K, SITES)
    base = jax.random.truncated_normal(key_base, -6.0, 6.0, shape, jnp.float32)
    scale = jnp.ones((TS, 1, 1, K, 1), jnp.float32)
    gains = jax.random.uniform(key_gain, (TS, 1, 1, K, 1), jnp.float32, 0.5, 1.5)
    phases = jax.random.uniform(key_phase, (TS, 1, 1, K, 1), jnp.float32, 0.0, 2.0 * math.pi)
    position = jnp.arange(SITES, dtype=jnp.float32) / SITES
    envelope = jnp.exp(gains * jnp.cos(2.0 * math.pi * position + phases))
    return (base * envelope * scale).astype(jnp.bfloat16)


def levels(rng, shape, pieces, least, top_value):
    factor_of, own = 1.0, jax.random.fold_in(rng, 6)
    for axis_at, shards_of in pieces:
        heights = jnp.exp(jax.random.uniform(jax.random.fold_in(own, axis_at), (shards_of,), jnp.float32, least / len(pieces), top_value / len(pieces)))
        factor_of = factor_of * jnp.repeat(heights, shape[axis_at] // shards_of).reshape([-1 if axis == axis_at else 1 for axis in range(len(shape))])
    return factor_of


def gaussian(own_key, extent, width, bound, cuts=(), held_as=jnp.bfloat16):
    entries = jax.random.normal(own_key, extent, jnp.float32) * width
    if len(cuts) > 0:
        entries = levels(own_key, extent, cuts, -0.22, 0.18) * entries
    return jnp.clip(entries, min=-bound, max=bound).astype(held_as)


def setup_inputs(seed: int = 0, part: int = 0) -> dict:
    streams_of = jax.random.split(jax.random.key(seed), 3)
    part_splits = jax.random.split(jax.random.fold_in(streams_of[2], part), 3)
    return {
        "solutions": gaussian(part_splits[0], (TS, 2, COLORS, NCOL, SITES), 1.0, 6.0, ((4, 16),)),
        "eigvecs": draw_eigvecs(jax.random.fold_in(jax.random.fold_in(streams_of[2], part), 71), part),
    }


def one_slice(pair):
    vectors, fields = pair
    vf = vectors.astype(jnp.float32)
    sf = fields.astype(jnp.float32)
    hi = lax.Precision.HIGHEST
    real = jnp.einsum('rckx,rcnx->kn', vf, sf, precision=hi)
    imag = jnp.einsum('ckx,cnx->kn', vf[0], sf[1], precision=hi) - jnp.einsum('ckx,cnx->kn', vf[1], sf[0], precision=hi)
    sumsq = lax.optimization_barrier(jnp.sum(vf * vf, axis=(0, 1, 3)))
    scale = lax.rsqrt(jnp.maximum(sumsq, jnp.float32(SITES)))
    return jnp.stack((real, imag), axis=1) * scale[:, None, None]

def reference(solutions, eigvecs):
    result = lax.map(one_slice, (eigvecs, solutions))
    return jnp.transpose(result, (1, 0, 2, 3))
```

```python
import functools

import jax
import jax.numpy as jnp
from jax import lax
from jax.experimental import pallas as pl
from jax.experimental.pallas import tpu as pltpu
from jax.sharding import PartitionSpec as P

SHARES = (5, 5)
LANES = 128


def project_kernel(*refs, first, steps, before, tail, pairs, wide, deep, own):
    vec_hbm, sol_hbm, refs = refs[0], refs[1], refs[2:]
    norms_in, refs = (refs[0], refs[1:]) if before else (None, refs)
    count = pairs * wide
    outs, refs = refs[:count], refs[count:]
    norms_out, refs = (None, refs) if tail else (refs[0], refs[1:])
    vecs, sols, both, norms, vec_sems, sol_sems = refs
    _, parts, colors, rows, sites = vecs.shape
    cols = sols.shape[3]
    width = 2 * cols

    def vec_copy(t):
        return pltpu.make_async_copy(vec_hbm.at[first + t], vecs.at[t], vec_sems.at[t])

    def sol_copy(t):
        return pltpu.make_async_copy(sol_hbm.at[first + t], sols.at[t], sol_sems.at[t])

    for t in range(steps):
        vec_copy(t).start()
        sol_copy(t).start()

    inner = lax.axis_index("sol")
    mine = (inner % pairs, inner // pairs, lax.axis_index("blk"))

    def start_of(pair, across, along):
        row = (((mine[2] + along) % deep) * wide + (mine[1] + across) % wide) * pairs
        row = (row + (mine[0] + pair) % pairs) * own
        return pl.multiple_of(row, own)

    places = [(p, x, z) for p in range(pairs) for x in range(wide) for z in range(deep)]
    starts = [start_of(*at) for at in places]

    if before:
        norms[...] = norms_in[...]
    else:
        norms[...] = jnp.zeros(norms.shape, jnp.float32)
    lane = lax.broadcasted_iota(jnp.int32, norms.shape, 1)

    def step(t, carry):
        vec_copy(t).wait()
        sol_copy(t).wait()
        lhs = jnp.concatenate(
            [
                jnp.concatenate([vecs[t, r, c] for c in range(colors)], axis=-1)
                for r in range(parts)
            ],
            axis=0,
        )
        prods = []
        for r in range(parts):
            rhs = jnp.concatenate([sols[t, r, c] for c in range(colors)], axis=-1)
            prods.append(
                lax.dot_general(
                    lhs, rhs, (((1,), (1,)), ((), ())), preferred_element_type=jnp.float32
                )
            )
        both[:, :cols] = prods[0][:rows] + prods[1][rows:]
        both[:, cols:] = prods[1][:rows] - prods[0][rows:]
        total = jnp.zeros((rows, sites), jnp.float32)
        for r in range(parts):
            for c in range(colors):
                vec = vecs[t, r, c].astype(jnp.float32)
                total = total + vec * vec
        sumsq = jnp.sum(total, axis=-1, keepdims=True)
        norms[...] = jnp.where(lane == t + before, sumsq, norms[...])
        at = pl.multiple_of(t * width, LANES)
        for (pair, across, along), row in zip(places, starts):
            outs[pair * wide + across][along, :, pl.ds(at, width)] = both[pl.ds(row, own), :]
        return carry

    lax.fori_loop(0, steps, step, 0)
    if tail:
        for (pair, across, along), row in zip(places, starts):
            out = outs[pair * wide + across]
            out[along, :, steps * width :] = norms[pl.ds(row, own), :]
    else:
        norms_out[...] = norms[...]


def project(eigvecs, solutions, norms, first, steps, pairs, wide, deep, own):
    slices, parts, colors, rows, sites = eigvecs.shape
    cols = solutions.shape[3]
    lanes = pl.cdiv(slices, LANES) * LANES
    tail = first + steps == slices
    width = steps * 2 * cols + (lanes if tail else 0)
    body = functools.partial(
        project_kernel,
        first=first,
        steps=steps,
        before=first,
        tail=tail,
        pairs=pairs,
        wide=wide,
        deep=deep,
        own=own,
    )
    out_shape = [pltpu.VMEM((deep, own, width), jnp.float32)] * (pairs * wide)
    if not tail:
        out_shape.append(pltpu.VMEM((rows, lanes), jnp.float32))
    args = (eigvecs, solutions) if norms is None else (eigvecs, solutions, norms)
    in_specs = [pl.BlockSpec(memory_space=pl.ANY)] * 2
    if norms is not None:
        in_specs.append(pl.BlockSpec(memory_space=pltpu.VMEM))
    return pl.pallas_call(
        body,
        in_specs=in_specs,
        out_specs=[pl.BlockSpec(memory_space=pltpu.VMEM)] * len(out_shape),
        out_shape=out_shape,
        scratch_shapes=[
            pltpu.VMEM((steps, parts, colors, rows, sites), eigvecs.dtype),
            pltpu.VMEM((steps, parts, colors, cols, sites), solutions.dtype),
            pltpu.VMEM((rows, 2 * cols), jnp.float32),
            pltpu.VMEM((rows, lanes), jnp.float32),
            pltpu.SemaphoreType.DMA((steps,)),
            pltpu.SemaphoreType.DMA((steps,)),
        ],
        cost_estimate=pl.CostEstimate(
            flops=4 * steps * parts * colors * rows * cols * sites,
            transcendentals=0,
            bytes_accessed=2 * steps * parts * colors * (rows + cols) * sites,
        ),
        name="project",
    )(*args)


def shards(solutions, eigvecs):
    deep = lax.axis_size("blk")
    within = lax.axis_size("sol")
    pairs = 2 if within % 2 == 0 else 1
    wide = within // pairs
    slices, _, _, rows, sites = eigvecs.shape
    cols = solutions.shape[3]
    own = rows // (deep * within)
    floor_value = jnp.float32(sites * deep * within)
    swap = [(i, i // pairs * pairs + (i + 1) % pairs) for i in range(within)]

    def across_by(shift):
        return [(i, (i // pairs + shift) % wide * pairs + i % pairs) for i in range(within)]

    def along_by(shift):
        return [(i, (i + shift) % deep) for i in range(deep)]

    sizes = [slices * part // sum(SHARES) for part in SHARES[:-1]]
    sizes = [size for size in sizes if size > 0]
    sizes.append(slices - sum(sizes))
    norms, first, partial = None, 0, []
    for size in sizes:
        found = project(eigvecs, solutions, norms, first, size, pairs, wide, deep, own)
        partial.append(found[: pairs * wide])
        norms = found[-1]
        first += size
    sums = []
    for part in partial:
        held = list(part[:wide])
        if pairs == 2:
            for across in list(range(1, wide)) + [0]:
                held[across] = held[across] + lax.ppermute(part[wide + across], "sol", swap)
        summed = held[0]
        for across in range(1, wide):
            summed = summed + lax.ppermute(held[across], "sol", across_by(across))
        done = summed[0]
        for along in range(1, deep):
            done = done + lax.ppermute(summed[along], "blk", along_by(along))
        sums.append(done)
    squares = sums[-1][:, sizes[-1] * 2 * cols :][:, :slices]
    scale = lax.rsqrt(jnp.maximum(squares, floor_value))[:, :, None, None]
    values = [
        done[:, : size * 2 * cols].reshape(own, size, 2, cols) for done, size in zip(sums, sizes)
    ]
    return jnp.concatenate(values, axis=1) * scale


def solution(mesh):
    in_specs = (
        P("cuts", None, None, None, ("blk", "sol")),
        P("cuts", None, None, None, ("blk", "sol")),
    )
    out_specs = P(("blk", "sol"), "cuts", None, None)
    return jax.shard_map(shards, mesh=mesh, in_specs=in_specs, out_specs=out_specs, check_vma=False)
```

```python
import functools

import jax
import jax.numpy as jnp
from jax import lax
from jax.experimental import pallas as pl
from jax.experimental.pallas import tpu as pltpu
from jax.sharding import PartitionSpec as P

SHARES = (5, 5)
LANES = 128


def project_kernel(*refs, first, steps, before, tail, pairs, wide, deep, own):
    vec_hbm, sol_hbm, refs = refs[0], refs[1], refs[2:]
    norms_in, refs = (refs[0], refs[1:]) if before else (None, refs)
    count = pairs * wide
    outs, refs = refs[:count], refs[count:]
    norms_out, refs = (None, refs) if tail else (refs[0], refs[1:])
    vecs, sols, both, norms, vec_sems, sol_sems = refs
    _, parts, colors, rows, sites = vecs.shape
    cols = sols.shape[3]
    width = 2 * cols

    def vec_copy(t):
        return pltpu.make_async_copy(vec_hbm.at[first + t], vecs.at[t], vec_sems.at[t])

    def sol_copy(t):
        return pltpu.make_async_copy(sol_hbm.at[first + t], sols.at[t], sol_sems.at[t])

    for t in range(steps):
        vec_copy(t).start()
        sol_copy(t).start()

    inner = lax.axis_index("sol")
    mine = (inner % pairs, inner // pairs, lax.axis_index("blk"))

    def start_of(pair, across, along):
        row = (((mine[2] + along) % deep) * wide + (mine[1] + across) % wide) * pairs
        row = (row + (mine[0] + pair) % pairs) * own
        return pl.multiple_of(row, own)

    places = [(p, x, z) for p in range(pairs) for x in range(wide) for z in range(deep)]
    starts = [start_of(*at) for at in places]

    if before:
        norms[...] = norms_in[...]
    else:
        norms[...] = jnp.zeros(norms.shape, jnp.float32)
    lane = lax.broadcasted_iota(jnp.int32, norms.shape, 1)

    def step(t, carry):
        vec_copy(t).wait()
        sol_copy(t).wait()
        lhs = jnp.concatenate(
            [
                jnp.concatenate([vecs[t, r, c] for c in range(colors)], axis=-1)
                for r in range(parts)
            ],
            axis=0,
        )
        prods = []
        for r in range(parts):
            rhs = jnp.concatenate([sols[t, r, c] for c in range(colors)], axis=-1)
            prods.append(
                lax.dot_general(
                    lhs, rhs, (((1,), (1,)), ((), ())), preferred_element_type=jnp.float32
                )
            )
        both[:, :cols] = prods[0][:rows] + prods[1][rows:]
        both[:, cols:] = prods[1][:rows] - prods[0][rows:]
        total = jnp.zeros((rows, sites), jnp.float32)
        for r in range(parts):
            for c in range(colors):
                vec = vecs[t, r, c].astype(jnp.float32)
                total = total + vec * vec
        sumsq = jnp.sum(total, axis=-1, keepdims=True)
        norms[...] = jnp.where(lane == t + before, sumsq, norms[...])
        at = pl.multiple_of(t * width, LANES)
        for (pair, across, along), row in zip(places, starts):
            outs[pair * wide + across][along, :, pl.ds(at, width)] = both[pl.ds(row, own), :]
        return carry

    lax.fori_loop(0, steps, step, 0)
    if tail:
        for (pair, across, along), row in zip(places, starts):
            out = outs[pair * wide + across]
            out[along, :, steps * width :] = norms[pl.ds(row, own), :]
    else:
        norms_out[...] = norms[...]


def project(eigvecs, solutions, norms, first, steps, pairs, wide, deep, own):
    slices, parts, colors, rows, sites = eigvecs.shape
    cols = solutions.shape[3]
    lanes = pl.cdiv(slices, LANES) * LANES
    tail = first + steps == slices
    width = steps * 2 * cols + (lanes if tail else 0)
    body = functools.partial(
        project_kernel,
        first=first,
        steps=steps,
        before=first,
        tail=tail,
        pairs=pairs,
        wide=wide,
        deep=deep,
        own=own,
    )
    out_shape = [pltpu.VMEM((deep, own, width), jnp.float32)] * (pairs * wide)
    if not tail:
        out_shape.append(pltpu.VMEM((rows, lanes), jnp.float32))
    args = [eigvecs, solutions]
    if norms is not None:
        args.append(pltpu.with_memory_space_constraint(norms, pltpu.VMEM))
    in_specs = [pl.BlockSpec(memory_space=pl.ANY)] * 2
    if norms is not None:
        in_specs.append(pl.BlockSpec(memory_space=pltpu.VMEM))
    return pl.pallas_call(
        body,
        in_specs=in_specs,
        out_specs=[pl.BlockSpec(memory_space=pltpu.VMEM)] * len(out_shape),
        out_shape=out_shape,
        scratch_shapes=[
            pltpu.VMEM((steps, parts, colors, rows, sites), eigvecs.dtype),
            pltpu.VMEM((steps, parts, colors, cols, sites), solutions.dtype),
            pltpu.VMEM((rows, 2 * cols), jnp.float32),
            pltpu.VMEM((rows, lanes), jnp.float32),
            pltpu.SemaphoreType.DMA((steps,)),
            pltpu.SemaphoreType.DMA((steps,)),
        ],
        cost_estimate=pl.CostEstimate(
            flops=4 * steps * parts * colors * rows * cols * sites,
            transcendentals=0,
            bytes_accessed=2 * steps * parts * colors * (rows + cols) * sites,
        ),
        name="project",
    )(*args)


def shards(solutions, eigvecs):
    deep = lax.axis_size("blk")
    within = lax.axis_size("sol")
    pairs = 2 if within % 2 == 0 else 1
    wide = within // pairs
    slices, _, _, rows, sites = eigvecs.shape
    cols = solutions.shape[3]
    own = rows // (deep * within)
    floor_value = jnp.float32(sites * deep * within)
    swap = [(i, i // pairs * pairs + (i + 1) % pairs) for i in range(within)]

    def across_by(shift):
        return [(i, (i // pairs + shift) % wide * pairs + i % pairs) for i in range(within)]

    def along_by(shift):
        return [(i, (i + shift) % deep) for i in range(deep)]

    sizes = [slices * part // sum(SHARES) for part in SHARES[:-1]]
    sizes = [size for size in sizes if size > 0]
    sizes.append(slices - sum(sizes))
    norms, first, partial = None, 0, []
    for size in sizes:
        found = project(eigvecs, solutions, norms, first, size, pairs, wide, deep, own)
        partial.append(found[: pairs * wide])
        norms = found[-1]
        first += size
    sums = []
    for part in partial:
        held = list(part[:wide])
        if pairs == 2:
            for across in list(range(1, wide)) + [0]:
                held[across] = held[across] + lax.ppermute(part[wide + across], "sol", swap)
        summed = held[0]
        for across in range(1, wide):
            summed = summed + lax.ppermute(held[across], "sol", across_by(across))
        done = summed[0]
        for along in range(1, deep):
            done = done + lax.ppermute(summed[along], "blk", along_by(along))
        sums.append(done)
    squares = sums[-1][:, sizes[-1] * 2 * cols :][:, :slices]
    scale = lax.rsqrt(jnp.maximum(squares, floor_value))[:, :, None, None]
    values = [
        done[:, : size * 2 * cols].reshape(own, size, 2, cols) for done, size in zip(sums, sizes)
    ]
    return jnp.concatenate(values, axis=1) * scale


def solution(mesh):
    in_specs = (
        P("cuts", None, None, None, ("blk", "sol")),
        P("cuts", None, None, None, ("blk", "sol")),
    )
    out_specs = P(("blk", "sol"), "cuts", None, None)
    return jax.shard_map(shards, mesh=mesh, in_specs=in_specs, out_specs=out_specs, check_vma=False)
```
